32 devices in a mesh: row: 8 (over z, x), col: 4 (over y, core).
Axes of the slice: x: 2, y: 2, z: 4, core: 2. Of those that a mesh axis runs over, the one named last changes fastest.
Arguments:
- matrix: float32 [5, 8, 10, 4, 128, 128], P(None, 'row', None, 'col'), may hold values from 0 to 2.5, as said below
- flags: int32 [5, 8, 10, 4], P(None, 'row', None, 'col'), may hold values from 0 to 1, as said below
Outputs:
- factor: float32 [5, 8, 10, 4, 128, 128], P(None, 'row', None, 'col')
The draws below stay inside these ranges and needn't reach their ends.
Inputs may be any that keep to these rules, and one draw needn't show every extreme that they name: `matrix`: symmetric positive definite, of order 40*128, diagonal at least 1.5. `flags`: 0 marks a float32 tile, 1 a bfloat16 tile; every diagonal tile is 0.
All inputs are finite; a program needn't handle non-finite values.
Results may differ from the reference program's by a relative error of at most 0.0005.
The reference program's roundings to bfloat16 on the way count: a program that leaves them out, or rounds other values in their place, can miss the bound.
Values sent between devices are 32-bit elements; how exact they have to be, the bound alone decides.
A program may use at most 128 MiB of HBM per device.

```python
import jax
import jax.numpy as jnp
from jax import lax

B = 128
PT = 4
TR_DEV = 5
NT = 40
TC_DEV = 10


def draw_matrix(key, part):
    count = NT * B
    points = jax.random.uniform(jax.random.fold_in(key, 11), (count, 2), jnp.float32)
    order = jnp.argsort(points[:, 0])
    points = points[order]
    reach = 0.6
    nugget = 0.5
    delta_x = points[:, 0][:, None] - points[:, 0][None, :]
    delta_y = points[:, 1][:, None] - points[:, 1][None, :]
    dist = jnp.sqrt(delta_x * delta_x + delta_y * delta_y)
    cov = jnp.exp(-dist / reach) + nugget * jnp.eye(count, dtype=jnp.float32)
    tiled = cov.reshape(NT, B, NT, B).transpose(0, 2, 1, 3)
    return tiled.reshape(TR_DEV, NT // TR_DEV, TC_DEV, NT // TC_DEV, B, B)


def draw_flags(key, part):
    tile_ids = jnp.arange(NT, dtype=jnp.int32)
    spacing = jnp.abs(tile_ids[:, None] - tile_ids[None, :])
    band = jax.random.randint(jax.random.fold_in(key, 5), (), 2, 6)
    flips = jax.random.randint(jax.random.fold_in(key, 7), (NT, NT), 0, 4)
    far_mark = (flips != 0).astype(jnp.int32)
    near_mark = (flips == 0).astype(jnp.int32)
    marks = jnp.where(spacing == 0, 0, jnp.where(spacing >= band, far_mark, near_mark))
    return marks.astype(jnp.int32).reshape(TR_DEV, NT // TR_DEV, TC_DEV, NT // TC_DEV)


def setup_inputs(seed: int = 0) -> dict:
    key_list = jax.random.split(jax.random.key(seed), 3)
    matrix = draw_matrix(jax.random.fold_in(key_list[2], 71), 0)
    flags = draw_flags(jax.random.fold_in(key_list[2], 71), 0)
    return {"matrix": matrix, "flags": flags}


def storage_round(values):
    narrow = lax.optimization_barrier(values.astype(jnp.bfloat16))
    return narrow.astype(jnp.float32)

def reference(matrix, flags):
    width = PT * B
    tiles = matrix.reshape(NT, NT, B, B)
    marks = flags.reshape(NT, NT)
    work = jnp.where((marks == 1)[:, :, None, None], storage_round(tiles), tiles)
    tile_ids = jnp.arange(NT, dtype=jnp.int32)
    for step in range(2):
        start = step * PT
        rows = work[:, start:start + PT].transpose(0, 2, 1, 3).reshape(NT, B, width)
        dense = rows[start:start + PT].reshape(width, width)
        sym = jnp.tril(dense) + jnp.tril(dense, -1).T
        lower_block = jnp.linalg.cholesky(sym)
        flat = rows.reshape(NT * B, width)
        solved = jax.scipy.linalg.solve_triangular(lower_block, flat.T, lower=True).T.reshape(NT, B, width)
        solved = solved.at[start:start + PT].set(lower_block.reshape(PT, B, width))
        rounded = storage_round(solved)

        def row_update(args):
            tile_row, mark_row, index = args
            exact = jnp.einsum('ik,cjk->cij', solved[index], solved, precision=lax.Precision.HIGHEST)
            coarse = jnp.einsum('ik,cjk->cij', rounded[index], rounded, precision=lax.Precision.HIGHEST)
            live = (index >= tile_ids) & (tile_ids >= start + PT)
            updated = jnp.where((mark_row == 1)[:, None, None], tile_row - coarse, tile_row - exact)
            return jnp.where(live[:, None, None], updated, tile_row)
        work = lax.map(row_update, (work, marks, tile_ids))
        new_cols = solved.reshape(NT, B, PT, B).transpose(0, 2, 1, 3)
        keep = (tile_ids >= start)[:, None, None, None]
        work = work.at[:, start:start + PT].set(jnp.where(keep, new_cols, work[:, start:start + PT]))
    final = jnp.where((marks == 1)[:, :, None, None], storage_round(work), work)
    upper = tile_ids[:, None] < tile_ids[None, :]
    final = jnp.where(upper[:, :, None, None], jnp.float32(0.0), final)
    return final.reshape(TR_DEV, NT // TR_DEV, TC_DEV, NT // TC_DEV, B, B)
```

```python
import jax
import jax.numpy as jnp
from jax import lax
from jax.experimental import pallas as pl
from jax.experimental.pallas import tpu as pltpu
from jax.sharding import PartitionSpec as P

PT = 4
MICRO = 8
NT_DIMS = (((1,), (1,)), ((), ()))
TN_DIMS = (((0,), (0,)), ((), ()))


def dot_nt(a, b):
    return lax.dot_general(
        a, b, NT_DIMS, precision=lax.Precision.HIGHEST, preferred_element_type=jnp.float32
    )


def dot_nt_coarse(a, b):
    return lax.dot_general(
        a.astype(jnp.bfloat16),
        b.astype(jnp.bfloat16),
        NT_DIMS,
        preferred_element_type=jnp.float32,
    )


def factor_tile(start, work_ref, low_ref, inv_ref):
    tile = start.shape[0]
    lane = lax.broadcasted_iota(jnp.int32, (tile, tile), 1)
    sub = lax.broadcasted_iota(jnp.int32, (tile, tile), 0)
    work_ref[:, :tile] = start
    work_ref[:, tile:] = (lane == sub).astype(jnp.float32)
    lane8 = lax.broadcasted_iota(jnp.int32, (MICRO, tile), 1)
    sub8 = lax.broadcasted_iota(jnp.int32, (MICRO, tile), 0)

    def micro(p, carry):
        base = pl.multiple_of(p * MICRO, MICRO)
        both = work_ref[pl.ds(base, MICRO), :]
        turned = pltpu.roll(both[:, :tile], lax.rem(tile - base, tile), 1)
        s = {}
        for k in range(MICRO):
            for q in range(k + 1):
                s[k, q] = jnp.broadcast_to(turned[k : k + 1, q : q + 1], (1, 2 * tile))
        rows = [both[k : k + 1, :] for k in range(MICRO)]
        for q in range(MICRO):
            d = s[q, q]
            r = lax.rsqrt(d)
            r = r * (1.5 - 0.5 * d * r * r)
            rows[q] = rows[q] * r
            low = {k: s[k, q] * r for k in range(q + 1, MICRO)}
            for k in range(q + 1, MICRO):
                for m in range(q + 1, k + 1):
                    s[k, m] = s[k, m] - low[k] * low[m]
                rows[k] = rows[k] - low[k] * rows[q]
        done = jnp.concatenate(rows, axis=0)
        upper = jnp.where(lane8 >= base + sub8, done[:, :tile], 0.0)
        extra = done[:, tile:]
        low_ref[pl.ds(base, MICRO), :] = upper
        inv_ref[pl.ds(base, MICRO), :] = extra
        work_ref[...] -= lax.dot_general(
            upper,
            jnp.concatenate([upper, extra], axis=1),
            TN_DIMS,
            precision=lax.Precision.HIGHEST,
            preferred_element_type=jnp.float32,
        )
        return carry

    lax.fori_loop(0, tile // MICRO, micro, 0)


def factor_kernel(col_count, tile, grid_ref, low_ref, inv_ref, work_ref, up_ref):
    count = 2 * PT
    lane = lax.broadcasted_iota(jnp.int32, (tile, tile), 1)
    sub = lax.broadcasted_iota(jnp.int32, (tile, tile), 0)

    def span(i, j=None):
        return slice(i * tile, (i + 1 if j is None else j) * tile)

    for i in range(count):
        for j in range(i + 1):
            piece = grid_ref[i, j % col_count, j // col_count, :tile, :]
            if i == j:
                kept = jnp.where(lane <= sub, piece, 0.0)
                piece = kept + jnp.where(lane < sub, piece, 0.0).T
            low_ref[span(i), span(j)] = piece
        if i + 1 < count:
            low_ref[span(i), span(i + 1, count)] = jnp.zeros(
                (tile, (count - i - 1) * tile), jnp.float32
            )
    for t in range(count):
        stop = PT if t < PT else count
        if t == PT:
            for i in range(PT, count):
                left = low_ref[span(i), span(0, PT)]
                for j in range(PT, i + 1):
                    right = low_ref[span(j), span(0, PT)]
                    mark = grid_ref[i, j % col_count, j // col_count, tile : tile + 1, :]
                    taken = jnp.where(mark > 0.5, dot_nt_coarse(left, right), dot_nt(left, right))
                    low_ref[span(i), span(j)] -= taken
        factor_tile(low_ref[span(t), span(t)], work_ref, up_ref, inv_ref.at[t])
        low_ref[span(t), span(t)] = up_ref[...].T
        if t + 1 < count:
            solved = dot_nt(low_ref[span(t + 1, count), span(t)], inv_ref[t])
            low_ref[span(t + 1, count), span(t)] = solved
            for u in range(t + 1, stop):
                low_ref[span(u, count), span(u)] -= dot_nt(
                    low_ref[span(u, count), span(t)], low_ref[span(u), span(t)]
                )


def factor_blocks(grid):
    col_count = grid.shape[1]
    tile = grid.shape[4]
    count = 2 * PT
    return pl.pallas_call(
        lambda *refs: factor_kernel(col_count, tile, *refs),
        out_shape=(
            jax.ShapeDtypeStruct((count * tile, count * tile), jnp.float32),
            jax.ShapeDtypeStruct((count, tile, tile), jnp.float32),
        ),
        in_specs=[pl.BlockSpec(memory_space=pltpu.VMEM)],
        out_specs=(
            pl.BlockSpec(memory_space=pltpu.VMEM),
            pl.BlockSpec(memory_space=pltpu.VMEM),
        ),
        scratch_shapes=[
            pltpu.VMEM((tile, 2 * tile), jnp.float32),
            pltpu.VMEM((tile, tile), jnp.float32),
        ],
        cost_estimate=pl.CostEstimate(flops=40_000_000_000, bytes_accessed=9_000_000, transcendentals=0),
        name="factor_blocks",
    )(grid)


def solve_kernel(col_count, tile, ids_ref, panel_ref, low_ref, inv_ref, out_ref):
    count = 2 * PT
    row = ids_ref[pl.program_id(0)]

    def span(i, j=None):
        return slice(i * tile, (i + 1 if j is None else j) * tile)

    @pl.when(row < count)
    def _():
        base = pl.multiple_of(jnp.minimum(row, count - 1) * tile, tile)
        out_ref[0] = low_ref[pl.ds(base, tile), :]

    @pl.when(row >= count)
    def _():
        for step in range(2):
            first = step * PT
            if step == 1:
                before = out_ref[0, :, span(0, PT)]
                other = low_ref[span(PT, count), span(0, PT)]
                exact = dot_nt(before, other)
                coarse = dot_nt_coarse(before, other)
            for t in range(first, first + PT):
                value = panel_ref[t % col_count, 0, t // col_count, :tile, :]
                if step == 1:
                    mark = panel_ref[t % col_count, 0, t // col_count, tile : tile + 1, :]
                    value = value - jnp.where(
                        mark > 0.5, coarse[:, span(t - PT)], exact[:, span(t - PT)]
                    )
                if t > first:
                    value = value - dot_nt(
                        out_ref[0, :, span(first, t)], low_ref[span(t), span(first, t)]
                    )
                out_ref[0, :, span(t)] = dot_nt(value, inv_ref[t])


def solve_panels(ids, panels, low, inv, groups):
    col_count = panels.shape[0] // groups
    _, rows, slots, height, tile = panels.shape
    count = 2 * PT
    total = rows * groups
    return pl.pallas_call(
        lambda *refs: solve_kernel(col_count, tile, *refs),
        grid_spec=pltpu.PrefetchScalarGridSpec(
            num_scalar_prefetch=1,
            grid=(total,),
            in_specs=[
                pl.BlockSpec(
                    (col_count, 1, slots, height, tile),
                    lambda g, ids: (g % groups, g // groups, 0, 0, 0),
                ),
                pl.BlockSpec((count * tile, count * tile), lambda g, ids: (0, 0)),
                pl.BlockSpec((count, tile, tile), lambda g, ids: (0, 0, 0)),
            ],
            out_specs=pl.BlockSpec((1, tile, count * tile), lambda g, ids: (g, 0, 0)),
        ),
        out_shape=jax.ShapeDtypeStruct((total, tile, count * tile), jnp.float32),
        cost_estimate=pl.CostEstimate(
            flops=total * 800_000_000, bytes_accessed=total * 1_000_000, transcendentals=0
        ),
        name="solve_panels",
    )(ids, panels, low, inv)


def update_kernel(tile, rows_ref, cols_ref, marks_ref, raw_ref, left_ref, right_ref, out_ref):
    count = 2 * PT
    a = pl.program_id(0)
    b = pl.program_id(1)
    i = rows_ref[a]
    j = cols_ref[b]
    mark = marks_ref[a * pl.num_programs(1) + b]

    def rounded(value):
        return value.astype(jnp.bfloat16).astype(jnp.float32)

    @pl.when(i < j)
    def _():
        out_ref[...] = jnp.zeros_like(out_ref)

    @pl.when((i >= j) & (j < count))
    def _():
        base = pl.multiple_of(jnp.minimum(j, count - 1) * tile, tile)
        value = left_ref[a, :, pl.ds(base, tile)]
        out_ref[0, 0] = jnp.where(mark == 1, rounded(value), value)

    @pl.when((i >= j) & (j >= count) & (mark == 1))
    def _():
        value = rounded(raw_ref[0, 0]) - dot_nt_coarse(left_ref[a], right_ref[b])
        out_ref[0, 0] = rounded(value)

    @pl.when((i >= j) & (j >= count) & (mark != 1))
    def _():
        out_ref[0, 0] = raw_ref[0, 0] - dot_nt(left_ref[a], right_ref[b])


def update_tiles(row_ids, col_ids, marks, tiles, left, right):
    rows, cols, tile, _ = tiles.shape
    whole = lambda a, b, *refs: (0, 0, 0)
    each = lambda a, b, *refs: (a, b, 0, 0)
    return pl.pallas_call(
        lambda *refs: update_kernel(tile, *refs),
        grid_spec=pltpu.PrefetchScalarGridSpec(
            num_scalar_prefetch=3,
            grid=(rows, cols),
            in_specs=[
                pl.BlockSpec((1, 1, tile, tile), each),
                pl.BlockSpec(left.shape, whole),
                pl.BlockSpec(right.shape, whole),
            ],
            out_specs=pl.BlockSpec((1, 1, tile, tile), each),
        ),
        out_shape=jax.ShapeDtypeStruct(tiles.shape, jnp.float32),
        compiler_params=pltpu.CompilerParams(vmem_limit_bytes=60 * 1024 * 1024),
        name="update_tiles",
    )(row_ids, col_ids, marks.reshape(-1), tiles, left, right)


def on_device(matrix, flags):
    row_count = lax.axis_size("row")
    col_count = lax.axis_size("col")
    row_index = lax.axis_index("row")
    col_index = lax.axis_index("col")
    tile_rows = matrix.shape[0]
    tile_cols = matrix.shape[2]
    tile = matrix.shape[4]
    count = 2 * PT
    slots = count // col_count
    groups = row_count // col_count
    tiles = matrix.reshape(tile_rows, tile_cols, tile, tile)
    marks = flags.reshape(tile_rows, tile_cols)
    row_ids = jnp.arange(tile_rows, dtype=jnp.int32) * row_count + row_index
    col_ids = jnp.arange(tile_cols, dtype=jnp.int32) * col_count + col_index

    head = tiles[:, :slots]
    head_marks = (marks[:, :slots] == 1)[:, :, None, None]
    stored = jnp.where(head_marks, lax.reduce_precision(head, 8, 7), head)
    tags = jnp.broadcast_to(head_marks.astype(jnp.float32), (tile_rows, slots, 8, tile))
    payload = jnp.concatenate([stored, tags], axis=2)

    grid = lax.all_gather(payload[0], ("row", "col"))
    grid = grid.reshape(row_count, col_count, slots, tile + 8, tile)[:count]
    low, inv = factor_blocks(grid)

    perm = []
    for h in range(groups):
        for u in range(col_count):
            for v in range(col_count):
                source = (h * col_count + u) * col_count + v
                perm.append((source, (h * col_count + v) * col_count + u))
    swapped = lax.ppermute(payload, ("row", "col"), perm)
    own = lax.all_gather(payload, "col")
    across = lax.all_gather(swapped, "row")

    left = solve_panels(row_ids, own, low, inv, 1)
    right = solve_panels(col_ids, across, low, inv, groups)
    out = update_tiles(row_ids, col_ids, marks, tiles, left, right)
    return out.reshape(matrix.shape)


def solution(mesh):
    return jax.shard_map(
        on_device,
        mesh=mesh,
        in_specs=(P(None, "row", None, "col", None, None), P(None, "row", None, "col")),
        out_specs=P(None, "row", None, "col", None, None),
        check_vma=False,
    )
```

```python
import jax
import jax.numpy as jnp
from jax import lax
from jax.experimental import pallas as pl
from jax.experimental.pallas import tpu as pltpu
from jax.sharding import PartitionSpec as P

PT = 4
MICRO = 16
NT_DIMS = (((1,), (1,)), ((), ()))
TN_DIMS = (((0,), (0,)), ((), ()))


def dot_nt(a, b):
    return lax.dot_general(
        a, b, NT_DIMS, precision=lax.Precision.HIGHEST, preferred_element_type=jnp.float32
    )


def dot_nt_coarse(a, b):
    return lax.dot_general(
        a.astype(jnp.bfloat16),
        b.astype(jnp.bfloat16),
        NT_DIMS,
        preferred_element_type=jnp.float32,
    )


def split(value):
    high = value.astype(jnp.bfloat16)
    return high, (value - high.astype(jnp.float32)).astype(jnp.bfloat16)


def dot_bf16(a, b):
    return lax.dot_general(a, b, NT_DIMS, preferred_element_type=jnp.float32)


def dot_pairs(a, b):
    return dot_bf16(a[0], b[0]) + (dot_bf16(a[0], b[1]) + dot_bf16(a[1], b[0]))


def factor_tile(start, work_ref, low_ref, inv_ref):
    tile = start.shape[0]
    lane = lax.broadcasted_iota(jnp.int32, (tile, tile), 1)
    sub = lax.broadcasted_iota(jnp.int32, (tile, tile), 0)
    work_ref[:, :tile] = start
    work_ref[:, tile:] = (lane == sub).astype(jnp.float32)
    lane8 = lax.broadcasted_iota(jnp.int32, (MICRO, tile), 1)
    sub8 = lax.broadcasted_iota(jnp.int32, (MICRO, tile), 0)

    def micro(p, carry):
        base = pl.multiple_of(p * MICRO, MICRO)
        both = work_ref[pl.ds(base, MICRO), :]
        turned = pltpu.roll(both[:, :tile], lax.rem(tile - base, tile), 1)
        s = {}
        for k in range(MICRO):
            for q in range(k + 1):
                s[k, q] = jnp.broadcast_to(turned[k : k + 1, q : q + 1], (1, tile))
        rows = [both[k : k + 1, :tile] for k in range(MICRO)]
        more = [both[k : k + 1, tile:] for k in range(MICRO)]
        for q in range(MICRO):
            d = s[q, q]
            r = lax.rsqrt(d)
            r = r * (1.5 - 0.5 * d * r * r)
            rows[q] = rows[q] * r
            more[q] = more[q] * r
            low = {k: s[k, q] * r for k in range(q + 1, MICRO)}
            for k in range(q + 1, MICRO):
                for m in range(q + 1, k + 1):
                    s[k, m] = s[k, m] - low[k] * low[m]
                rows[k] = rows[k] - low[k] * rows[q]
                more[k] = more[k] - low[k] * more[q]
        upper = jnp.where(lane8 >= base + sub8, jnp.concatenate(rows, axis=0), 0.0)
        extra = jnp.concatenate(more, axis=0)
        low_ref[pl.ds(base, MICRO), :] = upper
        inv_ref[pl.ds(base, MICRO), :] = extra
        work_ref[...] -= lax.dot_general(
            upper,
            jnp.concatenate([upper, extra], axis=1),
            TN_DIMS,
            precision=lax.Precision.HIGHEST,
            preferred_element_type=jnp.float32,
        )
        return carry

    lax.fori_loop(0, tile // MICRO, micro, 0)


def factor_kernel(step, col_count, tile, grid_ref, *refs):
    if step:
        before_ref, low_ref, inv_ref, work_ref, up_ref = refs
    else:
        low_ref, inv_ref, work_ref, up_ref = refs
    first = step * PT
    count = 2 * PT - first
    lane = lax.broadcasted_iota(jnp.int32, (tile, tile), 1)
    sub = lax.broadcasted_iota(jnp.int32, (tile, tile), 0)

    def span(i, j=None):
        return slice(i * tile, (i + 1 if j is None else j) * tile)

    for i in range(count):
        for j in range(PT):
            if j > i:
                low_ref[span(i), span(j)] = jnp.zeros((tile, tile), jnp.float32)
                continue
            where = (first + i, (first + j) % col_count, j // col_count)
            piece = grid_ref[(*where, slice(0, tile))]
            if i == j:
                kept = jnp.where(lane <= sub, piece, 0.0)
                piece = kept + jnp.where(lane < sub, piece, 0.0).T
            if step:
                left = before_ref[span(PT + i), :]
                right = before_ref[span(PT + j), :]
                mark = grid_ref[(*where, slice(tile, tile + 1))]
                piece = piece - jnp.where(mark > 0.5, dot_nt_coarse(left, right), dot_nt(left, right))
            low_ref[span(i), span(j)] = piece
    for t in range(PT):
        factor_tile(low_ref[span(t), span(t)], work_ref, up_ref, inv_ref.at[t])
        low_ref[span(t), span(t)] = up_ref[...].T
        if t + 1 < count:
            solved = dot_nt(low_ref[span(t + 1, count), span(t)], inv_ref[t])
            low_ref[span(t + 1, count), span(t)] = solved
            for u in range(t + 1, PT):
                low_ref[span(u, count), span(u)] -= dot_nt(
                    low_ref[span(u, count), span(t)], low_ref[span(u), span(t)]
                )


def factor_blocks(step, grid, *before):
    col_count = grid.shape[1]
    tile = grid.shape[4]
    count = 2 * PT - step * PT
    vmem = pl.BlockSpec(memory_space=pltpu.VMEM)
    return pl.pallas_call(
        lambda *refs: factor_kernel(step, col_count, tile, *refs),
        out_shape=(
            jax.ShapeDtypeStruct((count * tile, PT * tile), jnp.float32),
            jax.ShapeDtypeStruct((PT, tile, tile), jnp.float32),
        ),
        in_specs=[vmem] * (1 + len(before)),
        out_specs=(vmem, vmem),
        scratch_shapes=[
            pltpu.VMEM((tile, 2 * tile), jnp.float32),
            pltpu.VMEM((tile, tile), jnp.float32),
        ],
        cost_estimate=pl.CostEstimate(flops=20_000_000_000, bytes_accessed=9_000_000, transcendentals=0),
        name="factor_blocks",
    )(grid, *before)


def solve_kernel(tile, groups, ids_ref, order_ref, panel_ref, low0_ref, inv0_ref, low1_ref, inv1_ref,
                 high_ref, rest_ref, low_h, low_l, inv_h, inv_l):
    count = 2 * PT
    width = PT * tile
    rows = panel_ref.shape[1]
    col_count = panel_ref.shape[0]
    group = pl.program_id(0)

    def span(i, j=None):
        return slice(i * tile, (i + 1 if j is None else j) * tile)

    @pl.when(group == 0)
    def _():
        for i in range(count):
            low_h[span(i), :width], low_l[span(i), :width] = split(low0_ref[span(i), :])
        for i in range(PT):
            at = PT + i
            low_h[span(at), width:], low_l[span(at), width:] = split(low1_ref[span(i), :])
            low_h[span(i), width:] = jnp.zeros((tile, width), jnp.bfloat16)
            low_l[span(i), width:] = jnp.zeros((tile, width), jnp.bfloat16)
            inv_h[i], inv_l[i] = split(inv0_ref[i])
            inv_h[at], inv_l[at] = split(inv1_ref[i])

    def flat(value):
        return value.reshape(rows * tile, tile)

    for t in range(count):
        first = t // PT * PT
        slot = t // col_count
        owner = order_ref[t]
        value = flat(panel_ref[owner, :, slot, :tile, :])
        if first:
            left = (high_ref[0, :, :width], rest_ref[0, :, :width])
            right = (low_h[span(t), :width], low_l[span(t), :width])
            coarse = dot_bf16(left[0], right[0])
            exact = coarse + (dot_bf16(left[0], right[1]) + dot_bf16(left[1], right[0]))
            mark = panel_ref[owner, :, slot, tile : tile + 1, :]
            mark = flat(jnp.broadcast_to(mark, (rows, tile, tile)))
            value = value - jnp.where(mark > 0.5, coarse, exact)
        if t > first:
            value = value - dot_pairs(
                (high_ref[0, :, span(first, t)], rest_ref[0, :, span(first, t)]),
                (low_h[span(t), span(first, t)], low_l[span(t), span(first, t)]),
            )
        high_ref[0, :, span(t)], rest_ref[0, :, span(t)] = split(
            dot_pairs(split(value), (inv_h[t], inv_l[t]))
        )

    row = ids_ref[group]

    @pl.when(row < count)
    def _():
        base = pl.multiple_of(jnp.minimum(row, count - 1) * tile, tile)
        high_ref[0, :tile, :] = low_h[pl.ds(base, tile), :]
        rest_ref[0, :tile, :] = low_l[pl.ds(base, tile), :]


def solve_panels(ids, order, panels, factors, groups):
    col_count = panels.shape[0] // groups
    _, rows, slots, height, tile = panels.shape
    count = 2 * PT
    full = count * tile
    keep = lambda n: (lambda g, *refs: (0,) * n)
    out_spec = pl.BlockSpec((1, rows * tile, full), lambda g, *refs: (g, 0, 0))
    out_shape = jax.ShapeDtypeStruct((groups, rows * tile, full), jnp.bfloat16)
    return pl.pallas_call(
        lambda *refs: solve_kernel(tile, groups, *refs),
        grid_spec=pltpu.PrefetchScalarGridSpec(
            num_scalar_prefetch=2,
            grid=(groups,),
            in_specs=[
                pl.BlockSpec((col_count, rows, slots, height, tile), lambda g, *refs: (g, 0, 0, 0, 0))
            ]
            + [pl.BlockSpec(f.shape, keep(len(f.shape))) for f in factors],
            out_specs=(out_spec, out_spec),
            scratch_shapes=[
                pltpu.VMEM((full, full), jnp.bfloat16),
                pltpu.VMEM((full, full), jnp.bfloat16),
                pltpu.VMEM((count, tile, tile), jnp.bfloat16),
                pltpu.VMEM((count, tile, tile), jnp.bfloat16),
            ],
        ),
        out_shape=(out_shape, out_shape),
        compiler_params=pltpu.CompilerParams(vmem_limit_bytes=56 * 1024 * 1024),
        cost_estimate=pl.CostEstimate(
            flops=groups * 4_000_000_000, bytes_accessed=groups * 6_000_000, transcendentals=0
        ),
        name="solve_panels",
    )(ids, order, panels, *factors)


def update_kernel(tile, groups, rows_ref, cols_ref, marks_ref, raw_ref, left_h, left_l, right_h, right_l, out_ref):
    count = 2 * PT
    b = pl.program_id(0)
    j = cols_ref[b]
    base = pl.multiple_of(jnp.minimum(j, count - 1) * tile, tile)
    at = pl.multiple_of(b // groups * tile, tile)
    group = b % groups

    def rounded(value):
        return value.astype(jnp.bfloat16).astype(jnp.float32)

    def tile_row(a):
        i = rows_ref[a]
        mark = marks_ref[a * pl.num_programs(0) + b]
        mine = slice(a * tile, (a + 1) * tile)

        @pl.when(i < j)
        def _():
            out_ref[a, 0] = jnp.zeros((tile, tile), jnp.float32)

        @pl.when((i >= j) & (j < count))
        def _():
            high = left_h[0, mine, pl.ds(base, tile)].astype(jnp.float32)
            rest = left_l[0, mine, pl.ds(base, tile)].astype(jnp.float32)
            out_ref[a, 0] = high + jnp.where(mark == 1, 0.0, rest)

        @pl.when((i >= j) & (j >= count) & (mark == 1))
        def _():
            other = right_h[group, pl.ds(at, tile), :]
            out_ref[a, 0] = rounded(rounded(raw_ref[a, 0]) - dot_bf16(left_h[0, mine, :], other))

        @pl.when((i >= j) & (j >= count) & (mark != 1))
        def _():
            high = right_h[group, pl.ds(at, tile), :]
            rest = right_l[group, pl.ds(at, tile), :]
            out_ref[a, 0] = raw_ref[a, 0] - dot_pairs(
                (left_h[0, mine, :], left_l[0, mine, :]), (high, rest)
            )

    for a in range(raw_ref.shape[0]):
        tile_row(a)


def update_tiles(row_ids, col_ids, marks, tiles, left, right):
    rows, cols, tile, _ = tiles.shape
    groups = right[0].shape[0]
    whole = lambda b, *refs: (0, 0, 0)
    each = pl.BlockSpec((rows, 1, tile, tile), lambda b, *refs: (0, b, 0, 0))
    return pl.pallas_call(
        lambda *refs: update_kernel(tile, groups, *refs),
        grid_spec=pltpu.PrefetchScalarGridSpec(
            num_scalar_prefetch=3,
            grid=(cols,),
            in_specs=[each] + [pl.BlockSpec(v.shape, whole) for v in (*left, *right)],
            out_specs=each,
        ),
        out_shape=jax.ShapeDtypeStruct(tiles.shape, jnp.float32),
        compiler_params=pltpu.CompilerParams(vmem_limit_bytes=60 * 1024 * 1024),
        name="update_tiles",
    )(row_ids, col_ids, marks.reshape(-1), tiles, *left, *right)


def on_device(matrix, flags):
    row_count = lax.axis_size("row")
    col_count = lax.axis_size("col")
    row_index = lax.axis_index("row")
    col_index = lax.axis_index("col")
    tile_rows = matrix.shape[0]
    tile_cols = matrix.shape[2]
    tile = matrix.shape[4]
    count = 2 * PT
    slots = count // col_count
    groups = row_count // col_count
    tiles = matrix.reshape(tile_rows, tile_cols, tile, tile)
    marks = flags.reshape(tile_rows, tile_cols)
    row_ids = jnp.arange(tile_rows, dtype=jnp.int32) * row_count + row_index
    col_ids = jnp.arange(tile_cols, dtype=jnp.int32) * col_count + col_index

    head = tiles[:, :slots]
    head_marks = (marks[:, :slots] == 1)[:, :, None, None]
    stored = jnp.where(head_marks, lax.reduce_precision(head, 8, 7), head)
    tags = jnp.broadcast_to(head_marks.astype(jnp.float32), (tile_rows, slots, 8, tile))
    payload = jnp.concatenate([stored, tags], axis=2)

    half = max(slots // 2, 1)
    grids = []
    for step in range(2 if slots > 1 else 1):
        piece = payload[0, step * half : (step + 1) * half]
        grid = lax.all_gather(piece, ("row", "col"))
        grids.append(grid.reshape(row_count, col_count, half, tile + 8, tile)[:count])
    low0, inv0 = factor_blocks(0, grids[0])
    low1, inv1 = factor_blocks(1, grids[-1], low0)
    factors = (low0, inv0, low1, inv1)

    perm = []
    for h in range(groups):
        for u in range(col_count):
            for v in range(col_count):
                source = (h * col_count + u) * col_count + v
                perm.append((source, (h * col_count + v) * col_count + u))
    swapped = lax.ppermute(payload, ("row", "col"), perm)
    pieces = [payload]
    for shift in range(1, col_count):
        ring = [(q, (q + shift) % col_count) for q in range(col_count)]
        pieces.append(lax.ppermute(payload, "col", ring))
    own = jnp.stack(pieces)
    across = lax.all_gather(swapped, "row")

    columns = jnp.arange(count, dtype=jnp.int32)
    turned = (col_index - columns + count * col_count) % col_count
    left = solve_panels(row_ids[:1], turned, own, factors, 1)
    right = solve_panels(col_ids[:groups], columns % col_count, across, factors, groups)
    out = update_tiles(row_ids, col_ids, marks, tiles, left, right)
    return out.reshape(matrix.shape)


def solution(mesh):
    return jax.shard_map(
        on_device,
        mesh=mesh,
        in_specs=(P(None, "row", None, "col", None, None), P(None, "row", None, "col")),
        out_specs=P(None, "row", None, "col", None, None),
        check_vma=False,
    )
```

```python
import jax
import jax.numpy as jnp
from jax import lax
from jax.experimental import pallas as pl
from jax.experimental.pallas import tpu as pltpu
from jax.sharding import PartitionSpec as P

PT = 4
MICRO = 16
NT_DIMS = (((1,), (1,)), ((), ()))
TN_DIMS = (((0,), (0,)), ((), ()))


def dot_nt(a, b):
    return lax.dot_general(
        a, b, NT_DIMS, precision=lax.Precision.HIGHEST, preferred_element_type=jnp.float32
    )


def dot_nt_coarse(a, b):
    return lax.dot_general(
        a.astype(jnp.bfloat16),
        b.astype(jnp.bfloat16),
        NT_DIMS,
        preferred_element_type=jnp.float32,
    )


def split(value):
    high = value.astype(jnp.bfloat16)
    return high, (value - high.astype(jnp.float32)).astype(jnp.bfloat16)


def dot_bf16(a, b):
    return lax.dot_general(a, b, NT_DIMS, preferred_element_type=jnp.float32)


def dot_pairs(a, b):
    return dot_bf16(a[0], b[0]) + (dot_bf16(a[0], b[1]) + dot_bf16(a[1], b[0]))


def factor_tile(start, work_ref, low_ref, inv_ref):
    tile = start.shape[0]
    lane = lax.broadcasted_iota(jnp.int32, (tile, tile), 1)
    sub = lax.broadcasted_iota(jnp.int32, (tile, tile), 0)
    work_ref[:, :tile] = start
    work_ref[:, tile:] = (lane == sub).astype(jnp.float32)
    lane8 = lax.broadcasted_iota(jnp.int32, (MICRO, tile), 1)
    sub8 = lax.broadcasted_iota(jnp.int32, (MICRO, tile), 0)

    def micro(p, carry):
        base = pl.multiple_of(p * MICRO, MICRO)
        both = work_ref[pl.ds(base, MICRO), :]
        turned = pltpu.roll(both[:, :tile], lax.rem(tile - base, tile), 1)
        s = {}
        for k in range(MICRO):
            for q in range(k + 1):
                s[k, q] = jnp.broadcast_to(turned[k : k + 1, q : q + 1], (1, tile))
        rows = [both[k : k + 1, :tile] for k in range(MICRO)]
        more = [both[k : k + 1, tile:] for k in range(MICRO)]
        for q in range(MICRO):
            d = s[q, q]
            r = lax.rsqrt(d)
            r = r * (1.5 - 0.5 * d * r * r)
            rows[q] = rows[q] * r
            more[q] = more[q] * r
            low = {k: s[k, q] * r for k in range(q + 1, MICRO)}
            for k in range(q + 1, MICRO):
                for m in range(q + 1, k + 1):
                    s[k, m] = s[k, m] - low[k] * low[m]
                rows[k] = rows[k] - low[k] * rows[q]
                more[k] = more[k] - low[k] * more[q]
        upper = jnp.where(lane8 >= base + sub8, jnp.concatenate(rows, axis=0), 0.0)
        extra = jnp.concatenate(more, axis=0)
        low_ref[pl.ds(base, MICRO), :] = upper
        inv_ref[pl.ds(base, MICRO), :] = extra
        work_ref[...] -= lax.dot_general(
            upper,
            jnp.concatenate([upper, extra], axis=1),
            TN_DIMS,
            precision=lax.Precision.HIGHEST,
            preferred_element_type=jnp.float32,
        )
        return carry

    lax.fori_loop(0, tile // MICRO, micro, 0)


def factor_kernel(step, col_count, tile, grid_ref, *refs):
    if step:
        before_ref, low_ref, inv_ref, work_ref, up_ref = refs
    else:
        low_ref, inv_ref, work_ref, up_ref = refs
    first = step * PT
    count = 2 * PT - first
    lane = lax.broadcasted_iota(jnp.int32, (tile, tile), 1)
    sub = lax.broadcasted_iota(jnp.int32, (tile, tile), 0)

    def span(i, j=None):
        return slice(i * tile, (i + 1 if j is None else j) * tile)

    for i in range(count):
        for j in range(PT):
            if j > i:
                low_ref[span(i), span(j)] = jnp.zeros((tile, tile), jnp.float32)
                continue
            where = (first + i, (first + j) % col_count, (first + j) // col_count)
            piece = grid_ref[(*where, slice(0, tile))]
            if i == j:
                kept = jnp.where(lane <= sub, piece, 0.0)
                piece = kept + jnp.where(lane < sub, piece, 0.0).T
            if step:
                left = before_ref[span(PT + i), :]
                right = before_ref[span(PT + j), :]
                mark = grid_ref[(*where, slice(tile, tile + 1))]
                piece = piece - jnp.where(mark > 0.5, dot_nt_coarse(left, right), dot_nt(left, right))
            low_ref[span(i), span(j)] = piece
    for t in range(PT):
        factor_tile(low_ref[span(t), span(t)], work_ref, up_ref, inv_ref.at[t])
        low_ref[span(t), span(t)] = up_ref[...].T
        if t + 1 < count:
            solved = dot_nt(low_ref[span(t + 1, count), span(t)], inv_ref[t])
            low_ref[span(t + 1, count), span(t)] = solved
            for u in range(t + 1, PT):
                low_ref[span(u, count), span(u)] -= dot_nt(
                    low_ref[span(u, count), span(t)], low_ref[span(u), span(t)]
                )


def factor_blocks(step, grid, *before):
    col_count = grid.shape[1]
    tile = grid.shape[4]
    count = 2 * PT - step * PT
    vmem = pl.BlockSpec(memory_space=pltpu.VMEM)
    return pl.pallas_call(
        lambda *refs: factor_kernel(step, col_count, tile, *refs),
        out_shape=(
            jax.ShapeDtypeStruct((count * tile, PT * tile), jnp.float32),
            jax.ShapeDtypeStruct((PT, tile, tile), jnp.float32),
        ),
        in_specs=[vmem] * (1 + len(before)),
        out_specs=(vmem, vmem),
        scratch_shapes=[
            pltpu.VMEM((tile, 2 * tile), jnp.float32),
            pltpu.VMEM((tile, tile), jnp.float32),
        ],
        cost_estimate=pl.CostEstimate(flops=20_000_000_000, bytes_accessed=9_000_000, transcendentals=0),
        name="factor_blocks",
    )(grid, *before)


def solve_kernel(tile, groups, ids_ref, order_ref, panel_ref, low0_ref, inv0_ref, low1_ref, inv1_ref,
                 high_ref, rest_ref, low_h, low_l, inv_h, inv_l):
    count = 2 * PT
    width = PT * tile
    rows = panel_ref.shape[1]
    col_count = panel_ref.shape[0]
    group = pl.program_id(0)

    def span(i, j=None):
        return slice(i * tile, (i + 1 if j is None else j) * tile)

    @pl.when(group == 0)
    def _():
        for i in range(count):
            low_h[span(i), :width], low_l[span(i), :width] = split(low0_ref[span(i), :])
        for i in range(PT):
            at = PT + i
            low_h[span(at), width:], low_l[span(at), width:] = split(low1_ref[span(i), :])
            low_h[span(i), width:] = jnp.zeros((tile, width), jnp.bfloat16)
            low_l[span(i), width:] = jnp.zeros((tile, width), jnp.bfloat16)
            inv_h[i], inv_l[i] = split(inv0_ref[i])
            inv_h[at], inv_l[at] = split(inv1_ref[i])

    def flat(value):
        return value.reshape(rows * tile, tile)

    for t in range(count):
        first = t // PT * PT
        slot = t // col_count
        owner = order_ref[t]
        value = flat(panel_ref[owner, :, slot, :tile, :])
        if first:
            left = (high_ref[0, :, :width], rest_ref[0, :, :width])
            right = (low_h[span(t), :width], low_l[span(t), :width])
            coarse = dot_bf16(left[0], right[0])
            exact = coarse + (dot_bf16(left[0], right[1]) + dot_bf16(left[1], right[0]))
            mark = panel_ref[owner, :, slot, tile : tile + 1, :]
            mark = flat(jnp.broadcast_to(mark, (rows, tile, tile)))
            value = value - jnp.where(mark > 0.5, coarse, exact)
        if t > first:
            value = value - dot_pairs(
                (high_ref[0, :, span(first, t)], rest_ref[0, :, span(first, t)]),
                (low_h[span(t), span(first, t)], low_l[span(t), span(first, t)]),
            )
        high_ref[0, :, span(t)], rest_ref[0, :, span(t)] = split(
            dot_pairs(split(value), (inv_h[t], inv_l[t]))
        )

    row = ids_ref[group]

    @pl.when(row < count)
    def _():
        base = pl.multiple_of(jnp.minimum(row, count - 1) * tile, tile)
        high_ref[0, :tile, :] = low_h[pl.ds(base, tile), :]
        rest_ref[0, :tile, :] = low_l[pl.ds(base, tile), :]


def solve_panels(ids, order, panels, factors, groups):
    col_count = panels.shape[0] // groups
    _, rows, slots, height, tile = panels.shape
    count = 2 * PT
    full = count * tile
    keep = lambda n: (lambda g, *refs: (0,) * n)
    out_spec = pl.BlockSpec((1, rows * tile, full), lambda g, *refs: (g, 0, 0))
    out_shape = jax.ShapeDtypeStruct((groups, rows * tile, full), jnp.bfloat16)
    return pl.pallas_call(
        lambda *refs: solve_kernel(tile, groups, *refs),
        grid_spec=pltpu.PrefetchScalarGridSpec(
            num_scalar_prefetch=2,
            grid=(groups,),
            in_specs=[
                pl.BlockSpec((col_count, rows, slots, height, tile), lambda g, *refs: (g, 0, 0, 0, 0))
            ]
            + [pl.BlockSpec(f.shape, keep(len(f.shape))) for f in factors],
            out_specs=(out_spec, out_spec),
            scratch_shapes=[
                pltpu.VMEM((full, full), jnp.bfloat16),
                pltpu.VMEM((full, full), jnp.bfloat16),
                pltpu.VMEM((count, tile, tile), jnp.bfloat16),
                pltpu.VMEM((count, tile, tile), jnp.bfloat16),
            ],
        ),
        out_shape=(out_shape, out_shape),
        compiler_params=pltpu.CompilerParams(vmem_limit_bytes=56 * 1024 * 1024),
        cost_estimate=pl.CostEstimate(
            flops=groups * 4_000_000_000, bytes_accessed=groups * 6_000_000, transcendentals=0
        ),
        name="solve_panels",
    )(ids, order, panels, *factors)


def update_kernel(tile, groups, rows_ref, cols_ref, marks_ref, raw_ref, left_h, left_l, right_h, right_l, out_ref):
    count = 2 * PT
    b = pl.program_id(0)
    j = cols_ref[b]
    base = pl.multiple_of(jnp.minimum(j, count - 1) * tile, tile)
    at = pl.multiple_of(b // groups * tile, tile)
    group = b % groups

    def rounded(value):
        return value.astype(jnp.bfloat16).astype(jnp.float32)

    def tile_row(a):
        i = rows_ref[a]
        mark = marks_ref[a * pl.num_programs(0) + b]
        mine = slice(a * tile, (a + 1) * tile)

        @pl.when(i < j)
        def _():
            out_ref[a, 0] = jnp.zeros((tile, tile), jnp.float32)

        @pl.when((i >= j) & (j < count))
        def _():
            high = left_h[0, mine, pl.ds(base, tile)].astype(jnp.float32)
            rest = left_l[0, mine, pl.ds(base, tile)].astype(jnp.float32)
            out_ref[a, 0] = high + jnp.where(mark == 1, 0.0, rest)

        @pl.when((i >= j) & (j >= count) & (mark == 1))
        def _():
            other = right_h[group, pl.ds(at, tile), :]
            out_ref[a, 0] = rounded(rounded(raw_ref[a, 0]) - dot_bf16(left_h[0, mine, :], other))

        @pl.when((i >= j) & (j >= count) & (mark != 1))
        def _():
            high = right_h[group, pl.ds(at, tile), :]
            rest = right_l[group, pl.ds(at, tile), :]
            out_ref[a, 0] = raw_ref[a, 0] - dot_pairs(
                (left_h[0, mine, :], left_l[0, mine, :]), (high, rest)
            )

    for a in range(raw_ref.shape[0]):
        tile_row(a)


def update_tiles(row_ids, col_ids, marks, tiles, left, right):
    rows, cols, tile, _ = tiles.shape
    groups = right[0].shape[0]
    whole = lambda b, *refs: (0, 0, 0)
    each = pl.BlockSpec((rows, 1, tile, tile), lambda b, *refs: (0, b, 0, 0))
    return pl.pallas_call(
        lambda *refs: update_kernel(tile, groups, *refs),
        grid_spec=pltpu.PrefetchScalarGridSpec(
            num_scalar_prefetch=3,
            grid=(cols,),
            in_specs=[each] + [pl.BlockSpec(v.shape, whole) for v in (*left, *right)],
            out_specs=each,
        ),
        out_shape=jax.ShapeDtypeStruct(tiles.shape, jnp.float32),
        compiler_params=pltpu.CompilerParams(vmem_limit_bytes=60 * 1024 * 1024),
        name="update_tiles",
    )(row_ids, col_ids, marks.reshape(-1), tiles, *left, *right)


def on_device(matrix, flags):
    row_count = lax.axis_size("row")
    col_count = lax.axis_size("col")
    row_index = lax.axis_index("row")
    col_index = lax.axis_index("col")
    tile_rows = matrix.shape[0]
    tile_cols = matrix.shape[2]
    tile = matrix.shape[4]
    count = 2 * PT
    slots = count // col_count
    groups = row_count // col_count
    tiles = matrix.reshape(tile_rows, tile_cols, tile, tile)
    marks = flags.reshape(tile_rows, tile_cols)
    row_ids = jnp.arange(tile_rows, dtype=jnp.int32) * row_count + row_index
    col_ids = jnp.arange(tile_cols, dtype=jnp.int32) * col_count + col_index

    head = tiles[:, :slots]
    head_marks = (marks[:, :slots] == 1)[:, :, None, None]
    stored = jnp.where(head_marks, lax.reduce_precision(head, 8, 7), head)
    tags = jnp.broadcast_to(head_marks.astype(jnp.float32), (tile_rows, slots, 8, tile))
    payload = jnp.concatenate([stored, tags], axis=2)

    grid = lax.all_gather(payload[0], ("row", "col"))
    grid = grid.reshape(row_count, col_count, slots, tile + 8, tile)[:count]
    low0, inv0 = factor_blocks(0, grid)
    low1, inv1 = factor_blocks(1, grid, low0)
    factors = (low0, inv0, low1, inv1)

    perm = []
    for h in range(groups):
        for u in range(col_count):
            for v in range(col_count):
                source = (h * col_count + u) * col_count + v
                perm.append((source, (h * col_count + v) * col_count + u))
    swapped = lax.ppermute(payload, ("row", "col"), perm)
    pieces = [payload]
    for shift in range(1, col_count):
        ring = [(q, (q + shift) % col_count) for q in range(col_count)]
        pieces.append(lax.ppermute(payload, "col", ring))
    own = jnp.stack(pieces)
    across = lax.all_gather(swapped, "row")

    columns = jnp.arange(count, dtype=jnp.int32)
    turned = (col_index - columns + count * col_count) % col_count
    left = solve_panels(row_ids[:1], turned, own, factors, 1)
    right = solve_panels(col_ids[:groups], columns % col_count, across, factors, groups)
    out = update_tiles(row_ids, col_ids, marks, tiles, left, right)
    return out.reshape(matrix.shape)


def solution(mesh):
    return jax.shard_map(
        on_device,
        mesh=mesh,
        in_specs=(P(None, "row", None, "col", None, None), P(None, "row", None, "col")),
        out_specs=P(None, "row", None, "col", None, None),
        check_vma=False,
    )
```
